32 devices in a mesh: dp: 4 (over x, core), expert: 8 (over z, y).
Axes of the slice: x: 2, y: 2, z: 4, core: 2. Of those that a mesh axis runs over, the one named last changes fastest.
Arguments:
- tokens: bfloat16 [1024, 6144], P('dp', 'expert'), may hold values from -6 to 6
- cotangent: bfloat16 [1024, 6144], P('dp', 'expert'), may hold values from -6 to 6
- expert_choice: int32 [1024, 2], P('dp'), may hold values from 0 to 3, all different within a row; in each aligned block of 256 rows (0 to 255, 256 to 511, ...) at most 160 rows name the same one
- gate_values: bfloat16 [1024, 2], P('dp'), may hold values from 0.099609375 to 1
- gate_weight: bfloat16 [4, 6144, 2048], P('dp', None, 'expert'), may hold values from -0.078125 to 0.078125
- up_weight: bfloat16 [4, 6144, 2048], P('dp', None, 'expert'), may hold values from -0.078125 to 0.078125
- down_weight: bfloat16 [4, 2048, 6144], P('dp', 'expert'), may hold values from -0.125 to 0.125
- shrinker: bfloat16 [4, 32, 6144], P('dp'), may hold values from -0.078125 to 0.078125
- widener: bfloat16 [4, 2, 16, 2048], P('dp', None, None, 'expert'), may hold values from -0.375 to 0.375
- squeezer: bfloat16 [4, 16, 2048], P('dp', None, 'expert'), may hold values from -0.125 to 0.125
- spreader: bfloat16 [4, 16, 6144], P('dp'), may hold values from -0.375 to 0.375
Outputs:
- token_grad: bfloat16 [1024, 6144], P('dp', 'expert')
- gate_grad: float32 [1024, 2], P('dp')
- shrinker_grad: float32 [4, 32, 6144], P('dp')
- widener_grad: float32 [4, 2, 16, 2048], P('dp', None, None, 'expert')
- squeezer_grad: float32 [4, 16, 2048], P('dp', None, 'expert')
- spreader_grad: float32 [4, 16, 6144], P('dp')
The draws below stay inside these ranges and needn't reach their ends.
Inputs may be any that keep to these rules, and one draw needn't show every extreme that they name: `expert_choice`: each row names 2 different experts. Among the 256 tokens of one index of dp no expert is chosen more than 160 times, and some expert is chosen exactly 160 times by the tokens of some or all indices of dp.
All inputs are finite; a program needn't handle non-finite values.
Results may differ from the reference program's by a relative error of at most 0.02.
Values may be sent and summed in bfloat16 or wider, within the bound.
A program may use at most 128 MiB of HBM per device.

```python
import math
import jax
import jax.numpy as jnp
import numpy as np
from jax import lax

D = 6144
EXPERTS = 4
FF = 2048
RANK = 16
TOP = 2
TOK_DEV = 256
TOKENS = 1024
CAP = 160
N_DP = 4
N_EXPERT = 8


def steps_of(rng, extent, split, least, top_value):
    def one(dim, parts):
        steps = jax.random.uniform(jax.random.fold_in(jax.random.fold_in(rng, 6), dim), (parts,), jnp.float32, least / len(split), top_value / len(split))
        return jnp.repeat(jnp.exp(steps), extent[dim] // parts).reshape((-1,) + (1,) * (len(extent) - dim - 1))

    gain = one(*split[0])
    for cut in split[1:]:
        gain = gain * one(*cut)
    return gain


def shared_out(stream_key, own, number, rows, amount, top, bound, slope):
    ranking = jax.random.permutation(stream_key, amount)
    crowded, common = shares(amount, rows * top, bound, slope, True), shares(amount, rows * top, bound, slope, False)
    places = jnp.arange(amount)

    def named(sizes, rotation):
        used = int((sizes > 0).sum())
        fixed = max(1, used // 4)
        shifted = fixed + (places - fixed + rotation * (used - fixed)) % max(1, amount - fixed)
        return jnp.zeros((amount,), jnp.int32).at[ranking[jnp.where(places < fixed, places, shifted)]].set(jnp.asarray(sizes, jnp.int32))

    sizes = jnp.where(number % 4 == 0, named(crowded, number // 4), named(common, number - number // 4 - 1))
    mixed = jax.random.permutation(jax.random.fold_in(own, 3), amount)
    donor, receiver = mixed[0:amount // 2 * 2:2], mixed[1:amount // 2 * 2:2]
    slack = jnp.minimum(sizes[donor] - 1, bound - sizes[receiver]) // 2
    slack = jnp.where((donor == ranking[0]) | (receiver == ranking[0]) | (sizes[receiver] == 0), 0, jnp.maximum(slack, 0))
    shifted = jax.random.randint(jax.random.fold_in(own, 4), (amount // 2,), 0, 1 << 20) % (slack + 1)
    sizes = sizes.at[donor].add(-shifted).at[receiver].add(shifted)
    labels = jnp.searchsorted(jnp.cumsum(sizes), jnp.arange(rows * top), side="right").astype(jnp.int32)
    grid = labels.reshape(top, rows).T
    grid = grid[jax.random.permutation(jax.random.fold_in(own, 1), rows)]
    rotation = jax.random.randint(jax.random.fold_in(own, 2), (rows, 1), 0, top)
    return jnp.take_along_axis(grid, (jnp.arange(top)[None, :] + rotation) % top, axis=1)


def shares(count, total, most, slope, full):
    weights = [(1 << 20) // math.isqrt(standing ** slope) + 1 for standing in range(1, count + 1)]
    largest = most if full else min(most, max(-(-total // count), total * weights[0] // sum(weights)))
    least = 1 if total - largest >= count - 1 else 0
    holding, surplus = [largest] + [least] * (count - 1), total - largest - least * (count - 1)
    while surplus > 0:
        candidates = [i for i in range(1, count) if holding[i] < largest] or [i for i in range(1, count) if holding[i] < most]
        whole, budget = sum([weights[i] for i in candidates]), surplus
        for i in candidates:
            addition = min(most - holding[i], max(1, budget * weights[i] // whole), surplus)
            holding[i] = holding[i] + addition
            surplus = surplus - addition
    return np.array(holding)


def bell_draw(own_key, extent, spread, limit, split=(), kind=jnp.bfloat16):
    loudness = steps_of(own_key, extent, split, -0.22, 0.18) if split else 1.0
    drawn = jax.random.normal(own_key, extent, jnp.float32) * spread * loudness
    return jnp.minimum(jnp.maximum(drawn, -limit), limit).astype(kind)


def setup_inputs(seed: int = 0) -> dict:
    key_of = jax.random.split(jax.random.key(seed), 12)
    tokens = bell_draw(key_of[0], (TOKENS, D), 1.0, 6.0, ((0, 4), (1, 8)))
    cotangent = bell_draw(key_of[1], (TOKENS, D), 1.0, 6.0, ((0, 4), (1, 8)))
    expert_choice_keys = jax.random.split(jax.random.fold_in(key_of[2], 1), TOKENS // TOK_DEV)
    expert_choice_turns = jax.random.permutation(jax.random.fold_in(key_of[2], 3), TOKENS // TOK_DEV)
    expert_choice = jax.vmap(lambda own, number: shared_out(jax.random.fold_in(key_of[2], 2), own, number, TOK_DEV, EXPERTS, TOP, CAP, 2))(expert_choice_keys, expert_choice_turns).reshape((TOKENS, TOP))
    gate_values = jnp.clip(0.099609375 + 0.9003906 * jax.random.uniform(key_of[3], (TOKENS, TOP), jnp.float32) ** steps_of(key_of[3], (TOKENS, TOP), ((0, 4),), -0.2, 0.2), 0.099609375, 1.0).astype(jnp.bfloat16)
    gate_weight = bell_draw(key_of[4], (EXPERTS, D, FF), D ** -0.5, 0.078125, ((0, 4), (2, 8)))
    up_weight = bell_draw(key_of[5], (EXPERTS, D, FF), D ** -0.5, 0.078125, ((0, 4), (2, 8)))
    down_weight = bell_draw(key_of[6], (EXPERTS, FF, D), FF ** -0.5, 0.125, ((0, 4), (1, 8)))
    shrinker = bell_draw(key_of[7], (EXPERTS, 2 * RANK, D), D ** -0.5, 0.078125, ((0, 4),))
    widener = bell_draw(key_of[8], (EXPERTS, 2, RANK, FF), (16 * RANK) ** -0.5, 0.375, ((0, 4), (3, 8)))
    squeezer = bell_draw(key_of[9], (EXPERTS, RANK, FF), FF ** -0.5, 0.125, ((0, 4), (2, 8)))
    spreader = bell_draw(key_of[10], (EXPERTS, RANK, D), (16 * RANK) ** -0.5, 0.375, ((0, 4),))
    return dict(tokens=tokens, cotangent=cotangent, expert_choice=expert_choice, gate_values=gate_values, gate_weight=gate_weight, up_weight=up_weight, down_weight=down_weight, shrinker=shrinker, widener=widener, squeezer=squeezer, spreader=spreader)


adapter_scale = 2.0


def matmul(operand_a, operand_b):
    return jnp.dot(operand_a, operand_b, preferred_element_type=jnp.float32)


def silu_pair(gate_pre):
    logistic = jax.nn.sigmoid(gate_pre)
    return gate_pre * logistic, logistic * (1.0 + gate_pre * (1.0 - logistic))


def blockwise_grads(gate_delta, up_delta, gate_matrix, up_matrix):
    row_count = gate_delta.shape[0]
    ff_block = FF // N_EXPERT
    gate_parts = jnp.einsum("nkf,dkf->knd", gate_delta.astype(jnp.float32).reshape(row_count, N_EXPERT, ff_block), gate_matrix.astype(jnp.float32).reshape(D, N_EXPERT, ff_block))
    up_parts = jnp.einsum("nkf,dkf->knd", up_delta.astype(jnp.float32).reshape(row_count, N_EXPERT, ff_block), up_matrix.astype(jnp.float32).reshape(D, N_EXPERT, ff_block))
    rounded = lax.optimization_barrier((gate_parts + up_parts).astype(jnp.bfloat16))
    return jnp.sum(rounded.astype(jnp.float32), axis=0)


def reference(tokens, cotangent, expert_choice, gate_values, gate_weight, up_weight, down_weight, shrinker, widener, squeezer, spreader):
    blocks = N_DP
    per_block = TOK_DEV * TOP
    route_rows = expert_choice.reshape(blocks, per_block).astype(jnp.int32)
    onehot = (route_rows[:, :, None] == jnp.arange(EXPERTS, dtype=jnp.int32)[None, None, :]).astype(jnp.int32)
    before = (jnp.cumsum(onehot, axis=1) - onehot).astype(jnp.int32)
    slot_index = jnp.sum(before * onehot, axis=2).astype(jnp.int32)
    stacked = jnp.concatenate([tokens, cotangent], axis=1).astype(jnp.float32)
    stacked = jnp.repeat(stacked, TOP, axis=0).reshape(blocks, per_block, 2 * D)
    gate_rows = gate_values.reshape(blocks, per_block).astype(jnp.float32)
    slot_range = jnp.arange(CAP, dtype=jnp.int32)

    def per_expert(expert):
        chosen = ((route_rows[:, None, :] == expert) & (slot_index[:, None, :] == slot_range[None, :, None])).astype(jnp.float32)
        picked = jnp.einsum("bcj,bjd->bcd", chosen, stacked).reshape(blocks * CAP, 2 * D).astype(jnp.bfloat16)
        rows_x = picked[:, :D]
        rows_dy = picked[:, D:]
        rows_gate = jnp.sum(chosen * gate_rows[:, None, :], axis=2).reshape(blocks * CAP)
        lowrank_in = matmul(rows_x, shrinker[expert].T).astype(jnp.bfloat16)
        gate_pre = matmul(rows_x, gate_weight[expert]) + adapter_scale * matmul(lowrank_in[:, :RANK], widener[expert, 0])
        up_pre = matmul(rows_x, up_weight[expert]) + adapter_scale * matmul(lowrank_in[:, RANK:], widener[expert, 1])
        silu_gate, silu_slope = silu_pair(gate_pre)
        activation = (silu_gate * up_pre).astype(jnp.bfloat16)
        out_low = matmul(activation, squeezer[expert].T)
        low_out = out_low.astype(jnp.bfloat16)
        back_down = matmul(rows_dy, down_weight[expert].T)
        back_low = matmul(rows_dy, spreader[expert].T)
        gate_dots = jnp.sum(activation.astype(jnp.float32) * back_down, axis=1) + adapter_scale * jnp.sum(low_out.astype(jnp.float32) * back_low, axis=1)
        scaled_low = (rows_gate[:, None] * back_low).astype(jnp.bfloat16)
        act_delta = rows_gate[:, None] * back_down + adapter_scale * matmul(scaled_low, squeezer[expert])
        gate_delta = (act_delta * up_pre * silu_slope).astype(jnp.bfloat16)
        up_delta = (act_delta * silu_gate).astype(jnp.bfloat16)
        back_in = jnp.concatenate([matmul(gate_delta, widener[expert, 0].T), matmul(up_delta, widener[expert, 1].T)], axis=1).astype(jnp.bfloat16)
        row_grads = blockwise_grads(gate_delta, up_delta, gate_weight[expert], up_weight[expert]) + adapter_scale * matmul(back_in, shrinker[expert])
        shrink_grad = adapter_scale * matmul(back_in.T, rows_x)
        widen_grad = adapter_scale * jnp.stack([matmul(lowrank_in[:, :RANK].T, gate_delta), matmul(lowrank_in[:, RANK:].T, up_delta)])
        squeeze_grad = adapter_scale * matmul(scaled_low.T, activation)
        weighted_low = (rows_gate[:, None] * out_low).astype(jnp.bfloat16)
        spread_grad = adapter_scale * matmul(weighted_low.T, rows_dy)
        return row_grads, gate_dots, shrink_grad, widen_grad, squeeze_grad, spread_grad

    results = lax.map(per_expert, jnp.arange(EXPERTS, dtype=jnp.int32))
    row_grads, gate_dots, shrinker_grad, widener_grad, squeezer_grad, spreader_grad = results
    block_base = (jnp.arange(blocks, dtype=jnp.int32) * CAP)[:, None]
    position = (route_rows * (blocks * CAP) + block_base + slot_index).reshape(-1).astype(jnp.int32)
    picked_rows = jnp.take(row_grads.reshape(EXPERTS * blocks * CAP, D), position, axis=0)
    token_grad = jnp.sum(picked_rows.reshape(TOKENS, TOP, D), axis=1).astype(jnp.bfloat16)
    gate_grad = jnp.take(gate_dots.reshape(-1), position).reshape(TOKENS, TOP)
    return token_grad, gate_grad, shrinker_grad, widener_grad, squeezer_grad, spreader_grad
```

```python
import functools

import jax
import jax.numpy as jnp
from jax import lax
from jax.experimental import pallas as pl
from jax.experimental.pallas import tpu as pltpu
from jax.sharding import PartitionSpec as P

adapter_scale = 2.0
MESH = pl.DeviceIdType.MESH
tile_rows = 16


def product(pattern, operand_a, operand_b):
    return jnp.einsum(pattern, operand_a, operand_b, preferred_element_type=jnp.float32)


def silu_pair(gate_pre):
    logistic = jax.nn.sigmoid(gate_pre)
    return (gate_pre * logistic, logistic * (1.0 + gate_pre * (1.0 - logistic)))


def grid_of(n):
    inner = 1 << ((n.bit_length() - 1) // 2)
    return n // inner, inner


def ring_position(index, n):
    outer, inner = grid_of(n)
    span = inner - 1
    z, y = lax.div(index, inner), lax.rem(index, inner)
    odd = lax.rem(z, 2)
    walk = z * span + (1 - odd) * (y - 1) + odd * (span - y)
    back = outer * span + outer - 1 - z
    inside = lax.div(y + inner - 1, inner)
    return inside * walk + (1 - inside) * back


def ring_index(position, n):
    outer, inner = grid_of(n)
    span = inner - 1
    returning = lax.div(position, outer * span)
    z = lax.div(position, span)
    step = lax.rem(position, span)
    odd = lax.rem(z, 2)
    walk = z * inner + (1 - odd) * (1 + step) + odd * (span - step)
    back = (outer - 1 - (position - outer * span)) * inner
    return (1 - returning) * walk + returning * back


def meet(me_dp, me_ex, n_dp, left, right):
    barrier = pltpu.get_barrier_semaphore()
    for other in (left, right):
        pl.semaphore_signal(barrier, inc=1, device_id=(me_dp, other), device_id_type=MESH)
    for k in range(1, n_dp):
        peer = lax.rem(me_dp + k, n_dp)
        pl.semaphore_signal(barrier, inc=1, device_id=(peer, me_ex), device_id_type=MESH)
    pl.semaphore_wait(barrier, 2 + n_dp - 1)


def block_view(ref, row, rows, group, width, wide):
    rows_at = pl.ds(pl.multiple_of(row, tile_rows), rows)
    if wide:
        return ref.at[rows_at, pl.ds(pl.multiple_of(group * width, 128), width)]
    return ref.at[group, rows_at]


def gather_kernel(n, n_dp, cap, width, wide, x_ref, dy_ref, gate_ref, ox, ody, ogate,
                  local_sem, sent, came, ring_sent, ring_came):
    me_dp, me_ex = lax.axis_index("dp"), lax.axis_index("expert")
    here = ring_position(me_ex, n)
    around = [ring_index(lax.rem(here + j, n), n) for j in range(n)]
    right, left = around[1], around[n - 1]
    meet(me_dp, me_ex, n_dp, left, right)
    sources, outs = (x_ref, dy_ref), (ox, ody)

    def remote(src, dst, send_sem, recv_sem, dp, ex):
        return pltpu.make_async_remote_copy(
            src_ref=src, dst_ref=dst, send_sem=send_sem, recv_sem=recv_sem,
            device_id=(dp, ex), device_id_type=MESH)

    local, first, pending = [], {}, []
    for k in range(1, n_dp):
        peer = lax.rem(me_dp + k, n_dp)
        copy = remote(gate_ref.at[peer], ogate.at[me_dp], sent.at[2, k], came.at[2, k], peer, me_ex)
        copy.start()
        pending.append(copy)
    copy = pltpu.make_async_copy(gate_ref.at[me_dp], ogate.at[me_dp], local_sem.at[2])
    copy.start()
    local.append(copy)
    for a in range(2):
        for k in range(n_dp):
            peer = lax.rem(me_dp + k, n_dp)
            src = sources[a].at[pl.ds(pl.multiple_of(peer * cap, tile_rows), cap)]
            dst = block_view(outs[a], me_dp * cap, cap, me_ex, width, wide)
            if k == 0:
                copy = pltpu.make_async_copy(src, dst, local_sem.at[a])
            else:
                copy = remote(src, dst, sent.at[a, k], came.at[a, k], peer, me_ex)
            copy.start()
            first[a, k] = copy
    last = {}
    for s in range(n - 1):
        for a in range(2):
            for k in range(n_dp):
                if s > 0:
                    last[a, k].wait_recv()
                elif k > 0:
                    first[a, k].wait_recv()
                else:
                    first[a, k].wait()
                row = lax.rem(me_dp + n_dp - k, n_dp) * cap
                forward = k % 2 == 0
                group = around[(n - s) % n] if forward else around[s]
                view = block_view(outs[a], row, cap, group, width, wide)
                copy = remote(view, view, ring_sent.at[s, a, k], ring_came.at[s, a, k],
                              me_dp, right if forward else left)
                copy.start()
                last[a, k] = copy
                pending.append(copy)
    for a in range(2):
        for k in range(n_dp):
            last[a, k].wait_recv()
            if k > 0:
                first[a, k].wait_send()
    for copy in pending[:n_dp - 1]:
        copy.wait_recv()
    for copy in pending:
        copy.wait_send()
    local[0].wait()


def scatter_kernel(n, n_dp, cap, width, wide, term, extra, gate_ref, back, ogate,
                   slots, final, local_sem, sent, came, ring_sent, ring_came):
    me_dp, me_ex = lax.axis_index("dp"), lax.axis_index("expert")
    here = ring_position(me_ex, n)
    around = [ring_index(lax.rem(here + j, n), n) for j in range(n)]
    right, left = around[1], around[n - 1]
    meet(me_dp, me_ex, n_dp, left, right)

    def remote(src, dst, send_sem, recv_sem, dp, ex):
        return pltpu.make_async_remote_copy(
            src_ref=src, dst_ref=dst, send_sem=send_sem, recv_sem=recv_sem,
            device_id=(dp, ex), device_id_type=MESH)

    def own_part(row, group):
        at = pl.ds(pl.multiple_of(row, tile_rows), tile_rows)
        if wide:
            return term[at, pl.ds(pl.multiple_of(group * width, 128), width)].astype(jnp.float32)
        return term[group, at].astype(jnp.float32)

    pending, arrivals = [], []
    for k in range(1, n_dp):
        peer = lax.rem(me_dp + k, n_dp)
        copy = remote(gate_ref.at[peer], ogate.at[me_dp], sent.at[1, k], came.at[1, k], peer, me_ex)
        copy.start()
        pending.append(copy)
        arrivals.append(copy)
    own_gate = pltpu.make_async_copy(gate_ref.at[me_dp], ogate.at[me_dp], local_sem.at[1])
    own_gate.start()
    last = {}
    for s in range(n - 1):
        for k in range(n_dp):
            row = lax.rem(me_dp + k, n_dp) * cap
            rows_at = pl.ds(pl.multiple_of(row, tile_rows), cap)
            forward = k % 2 == 0
            group = around[(n - 1 - s) % n] if forward else around[(1 + s) % n]
            if s == 0:
                src = block_view(term, row, cap, group, width, wide)
            else:
                last[k].wait_recv()
                src = slots.at[s - 1, rows_at]

                def add(i, carry, row=row, group=group, s=s):
                    start = row + i * tile_rows
                    at = pl.ds(pl.multiple_of(start, tile_rows), tile_rows)
                    total = slots[s - 1, at].astype(jnp.float32) + own_part(start, group)
                    slots[s - 1, at] = total.astype(jnp.bfloat16)
                    return carry

                lax.fori_loop(0, cap // tile_rows, add, 0)
            copy = remote(src, slots.at[s, rows_at], ring_sent.at[s, k], ring_came.at[s, k],
                          me_dp, right if forward else left)
            copy.start()
            last[k] = copy
            pending.append(copy)
    own_rows = None
    for k in list(range(1, n_dp)) + [0]:
        peer = lax.rem(me_dp + k, n_dp)
        row = peer * cap
        last[k].wait_recv()

        def finish(i, carry, row=row):
            start = row + i * tile_rows
            at = pl.ds(pl.multiple_of(start, tile_rows), tile_rows)
            total = slots[n - 2, at].astype(jnp.float32) + own_part(start, me_ex) + extra[at]
            final[at] = total.astype(jnp.bfloat16)
            return carry

        lax.fori_loop(0, cap // tile_rows, finish, 0)
        src = final.at[pl.ds(pl.multiple_of(row, tile_rows), cap)]
        dst = back.at[pl.ds(pl.multiple_of(me_dp * cap, tile_rows), cap)]
        if k == 0:
            own_rows = pltpu.make_async_copy(src, dst, local_sem.at[0])
            own_rows.start()
        else:
            copy = remote(src, dst, sent.at[0, k], came.at[0, k], peer, me_ex)
            copy.start()
            pending.append(copy)
            arrivals.append(copy)
    for copy in arrivals:
        copy.wait_recv()
    for copy in pending:
        copy.wait_send()
    own_gate.wait()
    own_rows.wait()


def spread_rows(values, n_dp, cap):
    lanes = -(-cap // 128) * 128
    padded = jnp.pad(values.reshape(n_dp, 1, cap), ((0, 0), (0, 0), (0, lanes - cap)))
    return jnp.broadcast_to(padded, (n_dp, tile_rows, lanes)).astype(jnp.bfloat16)


def local(
    tokens,
    cotangent,
    expert_choice,
    gate_values,
    gate_weight,
    up_weight,
    down_weight,
    shrinker,
    widener,
    squeezer,
    spreader,
):
    tok_rows, width = tokens.shape
    top_k = expert_choice.shape[1]
    low_rank = spreader.shape[1]
    n = lax.axis_size("expert")
    n_dp = lax.axis_size("dp")
    cap = tok_rows * top_k * 5 // (4 * n_dp)
    own_rows = n_dp * cap
    wide = width % 128 == 0
    bf16, f32 = jnp.bfloat16, jnp.float32
    vmem = pl.BlockSpec(memory_space=pltpu.VMEM)
    anywhere = pl.BlockSpec(memory_space=pl.ANY)
    dma = pltpu.SemaphoreType.DMA

    flat_choice = expert_choice.reshape(-1)
    onehot = (flat_choice[:, None] == jnp.arange(n_dp, dtype=jnp.int32)[None, :]).astype(jnp.int32)
    before = jnp.cumsum(onehot, axis=0) - onehot
    slot_index = jnp.sum(before * onehot, axis=1)
    target = (flat_choice * cap + slot_index).reshape(tok_rows, top_k)
    row_ids = jnp.arange(own_rows, dtype=jnp.int32)
    hits = [target[None, :, k] == row_ids[:, None] for k in range(top_k)]
    placing = functools.reduce(jnp.logical_or, hits).astype(bf16)
    send_x = jnp.dot(placing, tokens, preferred_element_type=f32).astype(bf16)
    send_dy = jnp.dot(placing, cotangent, preferred_element_type=f32).astype(bf16)
    gates = gate_values.astype(f32)
    send_gate = sum(
        jnp.sum(jnp.where(hits[k], gates[None, :, k], 0.0), axis=1) for k in range(top_k)
    )
    gate_block = spread_rows(send_gate, n_dp, cap)
    whole = (own_rows, n * width) if wide else (n, own_rows, width)
    rows_x, rows_dy, gate_all = pl.pallas_call(
        functools.partial(gather_kernel, n, n_dp, cap, width, wide),
        out_shape=(
            jax.ShapeDtypeStruct(whole, bf16),
            jax.ShapeDtypeStruct(whole, bf16),
            jax.ShapeDtypeStruct(gate_block.shape, bf16),
        ),
        in_specs=[vmem] * 3,
        out_specs=(anywhere,) * 3,
        scratch_shapes=[
            dma((3,)),
            dma((3, n_dp)),
            dma((3, n_dp)),
            dma((n - 1, 2, n_dp)),
            dma((n - 1, 2, n_dp)),
        ],
        compiler_params=pltpu.CompilerParams(collective_id=0, has_side_effects=True),
    )(send_x, send_dy, gate_block)
    if not wide:
        rows_x = rows_x.transpose(1, 0, 2).reshape(own_rows, n * width)
        rows_dy = rows_dy.transpose(1, 0, 2).reshape(own_rows, n * width)
    gate_rows = gate_all[:, 0, :cap].reshape(-1).astype(f32)

    shrink_local = shrinker[0]
    widen_local = widener[0]
    squeeze_local = squeezer[0]
    spread_local = spreader[0]
    lowrank_in = product("nd,rd->nr", rows_x, shrink_local).astype(bf16)
    gate_pre = jnp.dot(
        rows_x, gate_weight[0], preferred_element_type=f32
    ) + adapter_scale * jnp.dot(
        lowrank_in[:, :low_rank], widen_local[0], preferred_element_type=f32
    )
    up_pre = jnp.dot(
        rows_x, up_weight[0], preferred_element_type=f32
    ) + adapter_scale * jnp.dot(
        lowrank_in[:, low_rank:], widen_local[1], preferred_element_type=f32
    )
    silu_gate, silu_slope = silu_pair(gate_pre)
    activation = (silu_gate * up_pre).astype(bf16)
    out_part = product("rf,nf->rn", squeeze_local, activation)
    back_down = product("nd,fd->nf", rows_dy, down_weight[0])
    back_low = product("rd,nd->rn", spread_local, rows_dy)
    gate_part = jnp.sum(activation.astype(f32) * back_down, axis=1)
    scaled_low = (back_low * gate_rows[None, :]).astype(bf16)
    act_delta = gate_rows[:, None] * back_down + adapter_scale * product(
        "rn,rf->nf", scaled_low, squeeze_local
    )
    gate_delta = (act_delta * up_pre * silu_slope).astype(bf16)
    up_delta = (act_delta * silu_gate).astype(bf16)
    parts = jnp.concatenate(
        [
            out_part,
            product("rf,nf->rn", widen_local[0], gate_delta),
            product("rf,nf->rn", widen_local[1], up_delta),
            gate_part[None],
        ],
        axis=0,
    ).astype(bf16)
    sums = lax.psum(parts, "expert")
    low_out = sums[:low_rank]
    out_low = low_out.astype(f32)
    back_in = sums[low_rank : 3 * low_rank]
    gate_dots = sums[3 * low_rank].astype(f32) + adapter_scale * jnp.sum(out_low * back_low, axis=0)
    term = (
        product("nf,df->nd", gate_delta, gate_weight[0])
        + product("nf,df->nd", up_delta, up_weight[0])
    ).astype(bf16)
    if not wide:
        term = term.reshape(own_rows, n, width).transpose(1, 0, 2)
    shrink_cols = lax.dynamic_slice_in_dim(
        shrink_local, lax.axis_index("expert") * width, width, 1
    )
    extra = adapter_scale * product("rn,rd->nd", back_in, shrink_cols)
    token_back, gate_back = pl.pallas_call(
        functools.partial(scatter_kernel, n, n_dp, cap, width, wide),
        out_shape=(
            jax.ShapeDtypeStruct((own_rows, width), bf16),
            jax.ShapeDtypeStruct(gate_block.shape, bf16),
        ),
        in_specs=[vmem] * 3,
        out_specs=(anywhere,) * 2,
        scratch_shapes=[
            pltpu.VMEM((n - 1, own_rows, width), bf16),
            pltpu.VMEM((own_rows, width), bf16),
            dma((2,)),
            dma((2, n_dp)),
            dma((2, n_dp)),
            dma((n - 1, n_dp)),
            dma((n - 1, n_dp)),
        ],
        compiler_params=pltpu.CompilerParams(
            collective_id=1, has_side_effects=True, vmem_limit_bytes=40 * 1024 * 1024
        ),
    )(term, extra, spread_rows(gate_dots, n_dp, cap))
    token_grad = product("rt,rd->td", placing, token_back).astype(bf16)
    gate_flat = gate_back[:, 0, :cap].reshape(own_rows).astype(f32)
    gate_grad = jnp.stack(
        [jnp.sum(jnp.where(hits[k], gate_flat[:, None], 0.0), axis=0) for k in range(top_k)],
        axis=1,
    )
    shrinker_grad = adapter_scale * product("rn,nd->rd", back_in, rows_x)
    widener_grad = adapter_scale * jnp.stack(
        [
            product("nr,nf->rf", lowrank_in[:, :low_rank], gate_delta),
            product("nr,nf->rf", lowrank_in[:, low_rank:], up_delta),
        ]
    )
    squeezer_grad = adapter_scale * product("rn,nf->rf", scaled_low, activation)
    weighted_low = (out_low * gate_rows[None, :]).astype(bf16)
    spreader_grad = adapter_scale * product("rn,nd->rd", weighted_low, rows_dy)
    return (
        token_grad,
        gate_grad,
        shrinker_grad[None],
        widener_grad[None],
        squeezer_grad[None],
        spreader_grad[None],
    )


def solution(mesh):
    placed = (
        P("dp", "expert"),
        P("dp", "expert"),
        P("dp", None),
        P("dp", None),
        P("dp", None, "expert"),
        P("dp", None, "expert"),
        P("dp", "expert", None),
        P("dp", None, None),
        P("dp", None, None, "expert"),
        P("dp", None, "expert"),
        P("dp", None, None),
    )
    return jax.shard_map(
        local,
        mesh=mesh,
        in_specs=placed,
        out_specs=(
            P("dp", "expert"),
            P("dp", None),
            P("dp", None, None),
            P("dp", None, None, "expert"),
            P("dp", None, "expert"),
            P("dp", None, None),
        ),
        check_vma=False,
    )
```

```python
import functools

import jax
import jax.numpy as jnp
from jax import lax
from jax.experimental import pallas as pl
from jax.experimental.pallas import tpu as pltpu
from jax.sharding import PartitionSpec as P

adapter_scale = 2.0
MESH = pl.DeviceIdType.MESH
tile_rows = 16


def product(pattern, operand_a, operand_b):
    return jnp.einsum(pattern, operand_a, operand_b, preferred_element_type=jnp.float32)


def silu_pair(gate_pre):
    logistic = jax.nn.sigmoid(gate_pre)
    return (gate_pre * logistic, logistic * (1.0 + gate_pre * (1.0 - logistic)))


def grid_of(n):
    inner = 1 << ((n.bit_length() - 1) // 2)
    return n // inner, inner


def ring_position(index, n):
    outer, inner = grid_of(n)
    span = inner - 1
    z, y = lax.div(index, inner), lax.rem(index, inner)
    odd = lax.rem(z, 2)
    walk = z * span + (1 - odd) * (y - 1) + odd * (span - y)
    back = outer * span + outer - 1 - z
    inside = lax.div(y + inner - 1, inner)
    return inside * walk + (1 - inside) * back


def ring_index(position, n):
    outer, inner = grid_of(n)
    span = inner - 1
    returning = lax.div(position, outer * span)
    z = lax.div(position, span)
    step = lax.rem(position, span)
    odd = lax.rem(z, 2)
    walk = z * inner + (1 - odd) * (1 + step) + odd * (span - step)
    back = (outer - 1 - (position - outer * span)) * inner
    return (1 - returning) * walk + returning * back


def meet(me_dp, me_ex, n_dp, left, right):
    barrier = pltpu.get_barrier_semaphore()
    for other in (left, right):
        pl.semaphore_signal(barrier, inc=1, device_id=(me_dp, other), device_id_type=MESH)
    for k in range(1, n_dp):
        peer = lax.rem(me_dp + k, n_dp)
        pl.semaphore_signal(barrier, inc=1, device_id=(peer, me_ex), device_id_type=MESH)
    pl.semaphore_wait(barrier, 2 + n_dp - 1)


def block_view(ref, row, rows, group, width, wide):
    rows_at = pl.ds(pl.multiple_of(row, tile_rows), rows)
    if wide:
        return ref.at[rows_at, pl.ds(pl.multiple_of(group * width, 128), width)]
    return ref.at[group, rows_at]


def gather_kernel(n, n_dp, cap, width, wide, x_ref, dy_ref, gate_ref, ox, ody, ogate,
                  local_sem, sent, came, ring_sent, ring_came):
    me_dp, me_ex = lax.axis_index("dp"), lax.axis_index("expert")
    here = ring_position(me_ex, n)
    around = [ring_index(lax.rem(here + j, n), n) for j in range(n)]
    right, left = around[1], around[n - 1]
    meet(me_dp, me_ex, n_dp, left, right)
    sources, outs = (x_ref, dy_ref), (ox, ody)

    def remote(src, dst, send_sem, recv_sem, dp, ex):
        return pltpu.make_async_remote_copy(
            src_ref=src, dst_ref=dst, send_sem=send_sem, recv_sem=recv_sem,
            device_id=(dp, ex), device_id_type=MESH)

    local, first, pending = [], {}, []
    for k in range(1, n_dp):
        peer = lax.rem(me_dp + k, n_dp)
        copy = remote(gate_ref.at[peer], ogate.at[me_dp], sent.at[2, k], came.at[2, k], peer, me_ex)
        copy.start()
        pending.append(copy)
    copy = pltpu.make_async_copy(gate_ref.at[me_dp], ogate.at[me_dp], local_sem.at[2])
    copy.start()
    local.append(copy)
    for a in range(2):
        for k in range(n_dp):
            peer = lax.rem(me_dp + k, n_dp)
            src = sources[a].at[pl.ds(pl.multiple_of(peer * cap, tile_rows), cap)]
            dst = block_view(outs[a], me_dp * cap, cap, me_ex, width, wide)
            if k == 0:
                copy = pltpu.make_async_copy(src, dst, local_sem.at[a])
            else:
                copy = remote(src, dst, sent.at[a, k], came.at[a, k], peer, me_ex)
            copy.start()
            first[a, k] = copy
    last = {}
    for s in range(n - 1):
        for a in range(2):
            for k in range(n_dp):
                if s > 0:
                    last[a, k].wait_recv()
                elif k > 0:
                    first[a, k].wait_recv()
                else:
                    first[a, k].wait()
                row = lax.rem(me_dp + n_dp - k, n_dp) * cap
                forward = k % 2 == 0
                group = around[(n - s) % n] if forward else around[s]
                view = block_view(outs[a], row, cap, group, width, wide)
                copy = remote(view, view, ring_sent.at[s, a, k], ring_came.at[s, a, k],
                              me_dp, right if forward else left)
                copy.start()
                last[a, k] = copy
                pending.append(copy)
    for a in range(2):
        for k in range(n_dp):
            last[a, k].wait_recv()
            if k > 0:
                first[a, k].wait_send()
    for copy in pending[:n_dp - 1]:
        copy.wait_recv()
    for copy in pending:
        copy.wait_send()
    local[0].wait()


def scatter_kernel(n, n_dp, cap, width, gate_delta, up_delta, gate_weight, up_weight, extra,
                   gate_ref, back, ogate, slots, final, own, stage, local_sem, sent, came, ring_sent, ring_came):
    me_dp, me_ex = lax.axis_index("dp"), lax.axis_index("expert")
    here = ring_position(me_ex, n)
    around = [ring_index(lax.rem(here + j, n), n) for j in range(n)]
    right, left = around[1], around[n - 1]
    meet(me_dp, me_ex, n_dp, left, right)

    def remote(src, dst, send_sem, recv_sem, dp, ex):
        return pltpu.make_async_remote_copy(
            src_ref=src, dst_ref=dst, send_sem=send_sem, recv_sem=recv_sem,
            device_id=(dp, ex), device_id_type=MESH)

    def form_terms(even_group, odd_group):
        def piece(k, carry):
            row = pl.multiple_of(lax.rem(me_dp + k, n_dp) * cap, tile_rows)
            odd = lax.rem(k, 2)
            group = (1 - odd) * even_group + odd * odd_group
            rows_at = pl.ds(row, cap)
            columns = pl.ds(pl.multiple_of(group * width, tile_rows), width)
            dims = (((1,), (1,)), ((), ()))
            own[rows_at] = lax.dot_general(
                gate_delta[rows_at], gate_weight[columns], dims, preferred_element_type=jnp.float32
            ) + lax.dot_general(
                up_delta[rows_at], up_weight[columns], dims, preferred_element_type=jnp.float32
            )
            return carry

        lax.fori_loop(0, n_dp, piece, 0)

    pending, arrivals = [], []
    for k in range(1, n_dp):
        peer = lax.rem(me_dp + k, n_dp)
        copy = remote(gate_ref.at[peer], ogate.at[me_dp], sent.at[1, k], came.at[1, k], peer, me_ex)
        copy.start()
        pending.append(copy)
        arrivals.append(copy)
    own_gate = pltpu.make_async_copy(gate_ref.at[me_dp], ogate.at[me_dp], local_sem.at[1])
    own_gate.start()
    last = {}
    for s in range(n - 1):
        form_terms(around[(n - 1 - s) % n], around[(1 + s) % n])
        for k in range(n_dp):
            row = lax.rem(me_dp + k, n_dp) * cap
            rows_at = pl.ds(pl.multiple_of(row, tile_rows), cap)
            forward = k % 2 == 0
            if s == 0:
                src = stage.at[rows_at]

                def put(i, carry, row=row):
                    at = pl.ds(pl.multiple_of(row + i * tile_rows, tile_rows), tile_rows)
                    stage[at] = own[at].astype(jnp.bfloat16)
                    return carry

                lax.fori_loop(0, cap // tile_rows, put, 0)
            else:
                last[k].wait_recv()
                src = slots.at[s - 1, rows_at]

                def add(i, carry, row=row, s=s):
                    start = row + i * tile_rows
                    at = pl.ds(pl.multiple_of(start, tile_rows), tile_rows)
                    total = slots[s - 1, at].astype(jnp.float32) + own[at]
                    slots[s - 1, at] = total.astype(jnp.bfloat16)
                    return carry

                lax.fori_loop(0, cap // tile_rows, add, 0)
            copy = remote(src, slots.at[s, rows_at], ring_sent.at[s, k], ring_came.at[s, k],
                          me_dp, right if forward else left)
            copy.start()
            last[k] = copy
            pending.append(copy)
    form_terms(me_ex, me_ex)
    own_rows = None
    for k in list(range(1, n_dp)) + [0]:
        peer = lax.rem(me_dp + k, n_dp)
        row = peer * cap
        last[k].wait_recv()

        def finish(i, carry, row=row):
            start = row + i * tile_rows
            at = pl.ds(pl.multiple_of(start, tile_rows), tile_rows)
            total = slots[n - 2, at].astype(jnp.float32) + own[at] + extra[at]
            final[at] = total.astype(jnp.bfloat16)
            return carry

        lax.fori_loop(0, cap // tile_rows, finish, 0)
        src = final.at[pl.ds(pl.multiple_of(row, tile_rows), cap)]
        dst = back.at[pl.ds(pl.multiple_of(me_dp * cap, tile_rows), cap)]
        if k == 0:
            own_rows = pltpu.make_async_copy(src, dst, local_sem.at[0])
            own_rows.start()
        else:
            copy = remote(src, dst, sent.at[0, k], came.at[0, k], peer, me_ex)
            copy.start()
            pending.append(copy)
            arrivals.append(copy)
    for copy in arrivals:
        copy.wait_recv()
    for copy in pending:
        copy.wait_send()
    own_gate.wait()
    own_rows.wait()


def spread_rows(values, n_dp, cap):
    lanes = -(-cap // 128) * 128
    padded = jnp.pad(values.reshape(n_dp, 1, cap), ((0, 0), (0, 0), (0, lanes - cap)))
    return jnp.broadcast_to(padded, (n_dp, tile_rows, lanes)).astype(jnp.bfloat16)


def local(
    tokens,
    cotangent,
    expert_choice,
    gate_values,
    gate_weight,
    up_weight,
    down_weight,
    shrinker,
    widener,
    squeezer,
    spreader,
):
    tok_rows, width = tokens.shape
    top_k = expert_choice.shape[1]
    low_rank = spreader.shape[1]
    n = lax.axis_size("expert")
    n_dp = lax.axis_size("dp")
    cap = tok_rows * top_k * 5 // (4 * n_dp)
    own_rows = n_dp * cap
    wide = width % 128 == 0
    bf16, f32 = jnp.bfloat16, jnp.float32
    vmem = pl.BlockSpec(memory_space=pltpu.VMEM)
    anywhere = pl.BlockSpec(memory_space=pl.ANY)
    dma = pltpu.SemaphoreType.DMA

    flat_choice = expert_choice.reshape(-1)
    onehot = (flat_choice[:, None] == jnp.arange(n_dp, dtype=jnp.int32)[None, :]).astype(jnp.int32)
    before = jnp.cumsum(onehot, axis=0) - onehot
    slot_index = jnp.sum(before * onehot, axis=1)
    target = (flat_choice * cap + slot_index).reshape(tok_rows, top_k)
    row_ids = jnp.arange(own_rows, dtype=jnp.int32)
    hits = [target[None, :, k] == row_ids[:, None] for k in range(top_k)]
    placing = functools.reduce(jnp.logical_or, hits).astype(bf16)
    send_x = jnp.dot(placing, tokens, preferred_element_type=f32).astype(bf16)
    send_dy = jnp.dot(placing, cotangent, preferred_element_type=f32).astype(bf16)
    gates = gate_values.astype(f32)
    send_gate = sum(
        jnp.sum(jnp.where(hits[k], gates[None, :, k], 0.0), axis=1) for k in range(top_k)
    )
    gate_block = spread_rows(send_gate, n_dp, cap)
    whole = (own_rows, n * width) if wide else (n, own_rows, width)
    rows_x, rows_dy, gate_all = pl.pallas_call(
        functools.partial(gather_kernel, n, n_dp, cap, width, wide),
        out_shape=(
            jax.ShapeDtypeStruct(whole, bf16),
            jax.ShapeDtypeStruct(whole, bf16),
            jax.ShapeDtypeStruct(gate_block.shape, bf16),
        ),
        in_specs=[vmem] * 3,
        out_specs=(anywhere,) * 3,
        scratch_shapes=[
            dma((3,)),
            dma((3, n_dp)),
            dma((3, n_dp)),
            dma((n - 1, 2, n_dp)),
            dma((n - 1, 2, n_dp)),
        ],
        compiler_params=pltpu.CompilerParams(collective_id=0, has_side_effects=True),
    )(send_x, send_dy, gate_block)
    if not wide:
        rows_x = rows_x.transpose(1, 0, 2).reshape(own_rows, n * width)
        rows_dy = rows_dy.transpose(1, 0, 2).reshape(own_rows, n * width)
    gate_rows = gate_all[:, 0, :cap].reshape(-1).astype(f32)

    shrink_local = shrinker[0]
    widen_local = widener[0]
    squeeze_local = squeezer[0]
    spread_local = spreader[0]
    lowrank_in = product("nd,rd->nr", rows_x, shrink_local).astype(bf16)
    gate_pre = jnp.dot(
        rows_x, gate_weight[0], preferred_element_type=f32
    ) + adapter_scale * jnp.dot(
        lowrank_in[:, :low_rank], widen_local[0], preferred_element_type=f32
    )
    up_pre = jnp.dot(
        rows_x, up_weight[0], preferred_element_type=f32
    ) + adapter_scale * jnp.dot(
        lowrank_in[:, low_rank:], widen_local[1], preferred_element_type=f32
    )
    silu_gate, silu_slope = silu_pair(gate_pre)
    activation = (silu_gate * up_pre).astype(bf16)
    out_part = product("rf,nf->rn", squeeze_local, activation)
    back_down = product("nd,fd->nf", rows_dy, down_weight[0])
    back_low = product("rd,nd->rn", spread_local, rows_dy)
    gate_part = jnp.sum(activation.astype(f32) * back_down, axis=1)
    scaled_low = (back_low * gate_rows[None, :]).astype(bf16)
    act_delta = gate_rows[:, None] * back_down + adapter_scale * product(
        "rn,rf->nf", scaled_low, squeeze_local
    )
    gate_delta = (act_delta * up_pre * silu_slope).astype(bf16)
    up_delta = (act_delta * silu_gate).astype(bf16)
    parts = jnp.concatenate(
        [
            out_part,
            product("rf,nf->rn", widen_local[0], gate_delta),
            product("rf,nf->rn", widen_local[1], up_delta),
            gate_part[None],
        ],
        axis=0,
    ).astype(bf16)
    sums = lax.psum(parts, "expert")
    low_out = sums[:low_rank]
    out_low = low_out.astype(f32)
    back_in = sums[low_rank : 3 * low_rank]
    gate_dots = sums[3 * low_rank].astype(f32) + adapter_scale * jnp.sum(out_low * back_low, axis=0)
    shrink_cols = lax.dynamic_slice_in_dim(
        shrink_local, lax.axis_index("expert") * width, width, 1
    )
    extra = adapter_scale * product("rn,rd->nd", back_in, shrink_cols)
    token_back, gate_back = pl.pallas_call(
        functools.partial(scatter_kernel, n, n_dp, cap, width),
        out_shape=(
            jax.ShapeDtypeStruct((own_rows, width), bf16),
            jax.ShapeDtypeStruct(gate_block.shape, bf16),
        ),
        in_specs=[vmem] * 6,
        out_specs=(anywhere,) * 2,
        scratch_shapes=[
            pltpu.VMEM((n - 1, own_rows, width), bf16),
            pltpu.VMEM((own_rows, width), bf16),
            pltpu.VMEM((own_rows, width), f32),
            pltpu.VMEM((own_rows, width), bf16),
            dma((2,)),
            dma((2, n_dp)),
            dma((2, n_dp)),
            dma((n - 1, n_dp)),
            dma((n - 1, n_dp)),
        ],
        compiler_params=pltpu.CompilerParams(
            collective_id=1, has_side_effects=True, vmem_limit_bytes=40 * 1024 * 1024
        ),
    )(
        gate_delta, up_delta, gate_weight[0], up_weight[0], extra, spread_rows(gate_dots, n_dp, cap)
    )
    token_grad = product("rt,rd->td", placing, token_back).astype(bf16)
    gate_flat = gate_back[:, 0, :cap].reshape(own_rows).astype(f32)
    gate_grad = jnp.stack(
        [jnp.sum(jnp.where(hits[k], gate_flat[:, None], 0.0), axis=0) for k in range(top_k)],
        axis=1,
    )
    shrinker_grad = adapter_scale * product("rn,nd->rd", back_in, rows_x)
    widener_grad = adapter_scale * jnp.stack(
        [
            product("nr,nf->rf", lowrank_in[:, :low_rank], gate_delta),
            product("nr,nf->rf", lowrank_in[:, low_rank:], up_delta),
        ]
    )
    squeezer_grad = adapter_scale * product("rn,nf->rf", scaled_low, activation)
    weighted_low = (out_low * gate_rows[None, :]).astype(bf16)
    spreader_grad = adapter_scale * product("rn,nd->rd", weighted_low, rows_dy)
    return (
        token_grad,
        gate_grad,
        shrinker_grad[None],
        widener_grad[None],
        squeezer_grad[None],
        spreader_grad[None],
    )


def solution(mesh):
    placed = (
        P("dp", "expert"),
        P("dp", "expert"),
        P("dp", None),
        P("dp", None),
        P("dp", None, "expert"),
        P("dp", None, "expert"),
        P("dp", "expert", None),
        P("dp", None, None),
        P("dp", None, None, "expert"),
        P("dp", None, "expert"),
        P("dp", None, None),
    )
    return jax.shard_map(
        local,
        mesh=mesh,
        in_specs=placed,
        out_specs=(
            P("dp", "expert"),
            P("dp", None),
            P("dp", None, None),
            P("dp", None, None, "expert"),
            P("dp", None, "expert"),
            P("dp", None, None),
        ),
        check_vma=False,
    )
```
